256 devices in a mesh: dp: 256 (over y, x, z, core).
Axes of the slice: x: 4, y: 4, z: 8, core: 2. Of those that a mesh axis runs over, the one named last changes fastest.
Arguments:
- gradients: bfloat16 [256, 384, 4608], P('dp'), may hold values from -144 to 144
- owned_rows: int32 [256], replicated, may hold values from 1 to 3, 384 in all
- master: float32 [768, 4608], P('dp'), may hold values from -0.09375 to 0.09375
- first_moment: float32 [768, 4608], P('dp'), may hold values from -0.01171875 to 0.01171875
- second_moment: float32 [768, 4608], P('dp'), may hold values from 1.695421e-07 to 1.695421e-06
Outputs:
- new_master: float32 [768, 4608], P('dp')
- new_first: float32 [768, 4608], P('dp')
- new_second: float32 [768, 4608], P('dp')
- direction: float32 [768, 4608], P('dp')
- weights: bfloat16 [384, 4608], replicated
The draws below stay inside these ranges and needn't reach their ends.
Inputs may be any that keep to these rules, and one draw needn't show every extreme that they name: `owned_rows`: owners hold consecutive flat rows in owner order; the counts sum to 384 and some owner holds exactly 3.
All inputs are finite; a program needn't handle non-finite values.
Results may differ from the reference program's by a relative error of at most 0.001.
Values may be sent and summed in bfloat16 or wider, within the bound.
A program may use at most 128 MiB of HBM per device.

```python
import math
import jax
import jax.numpy as jnp
import numpy as np
from jax import lax

D = 4608
CAP = 3
STEP = 100
ROWS = 384
N_DP = 256


def draw_gradients(key, part):
    base_key, pair_key = jax.random.split(jax.random.fold_in(key, 17))
    rows = jnp.arange(ROWS, dtype=jnp.float32) / ROWS
    base = jnp.clip(jax.random.normal(base_key, (N_DP, ROWS, D), jnp.float32), -6.0, 6.0)
    scale = 1.0 + 5.0 * rows
    pairing = jax.random.permutation(pair_key, N_DP)
    blocks = jnp.arange(ROWS, dtype=jnp.int32) * N_DP // ROWS
    spike = jnp.where(blocks[None, :] == pairing[:, None], 4.0, 1.0)
    return (base * scale[None, :, None] * spike[:, :, None]).astype(jnp.bfloat16)


def steps_of(rng, shape, shards, least, largest):
    loudness = 1.0
    for position, parts in shards:
        draws = jax.random.uniform(jax.random.fold_in(jax.random.fold_in(rng, 6), position), (parts,), jnp.float32, least / len(shards), largest / len(shards))
        loudness = loudness * jnp.repeat(jnp.exp(draws), shape[position] // parts).reshape((-1,) + (1,) * (len(shape) - 1 - position))
    return loudness


def split_up(count, total, most, lean):
    portions = [(1 << 20) // math.isqrt(rank ** lean) + 1 for rank in range(2, count + 1)]
    rest, counts = total - most - (count - 1), [1] * (count - 1)
    while rest > 0:
        candidates = [i for i in range(count - 1) if counts[i] < most]
        whole, left = sum([portions[i] for i in candidates]), rest
        for i in candidates:
            more = min(most - counts[i], max(1, left * portions[i] // whole), rest)
            counts[i] = counts[i] + more
            rest = rest - more
    return np.array([most] + counts)


def ragged(own_key, amount, total, bound, skew):
    if amount == 2:
        one = jax.random.randint(own_key, (), max(1, total - bound), min(bound, total - 1) + 1)
        return jnp.stack([one, total - one])
    tallies = jnp.asarray(split_up(amount, total, bound, skew), jnp.int32)
    pairs = (amount - 1) // 2
    giver, receiver = tallies[1:1 + 2 * pairs:2], tallies[2:2 + 2 * pairs:2]
    room = jnp.minimum(giver - 1, bound - receiver)
    passed = jax.random.randint(jax.random.fold_in(own_key, 1), (pairs,), 0, 1 << 20) % (room + 1)
    tallies = tallies.at[1:1 + 2 * pairs:2].set(giver - passed).at[2:2 + 2 * pairs:2].set(receiver + passed)
    return tallies[jax.random.permutation(jax.random.fold_in(own_key, 2), amount)]


def bell_draw(key, extent, scale, bound, pieces=(), held_as=jnp.bfloat16):
    values = scale * jax.random.normal(key, extent, jnp.float32)
    if pieces:
        values = values * steps_of(key, extent, pieces, -0.22, 0.18)
    return jnp.clip(values, -bound, bound).astype(held_as)


def setup_inputs(seed: int = 0) -> dict:
    splits = jax.random.split(jax.random.key(seed), 6)
    gradients = draw_gradients(jax.random.fold_in(splits[5], 71), 0)
    owned_rows = ragged(splits[1], N_DP, ROWS, CAP, 2).astype(jnp.int32)
    master = bell_draw(splits[2], (N_DP * CAP, D), D ** -0.5, 0.09375, ((0, 256),), jnp.float32)
    first_moment = bell_draw(splits[3], (N_DP * CAP, D), (1.0 / (ROWS * D) ** 0.5), 0.01171875, ((0, 256),), jnp.float32)
    second_moment = jnp.clip(jnp.exp(math.log(1.6954210195763153e-06) - 2.3025851 * jax.random.uniform(splits[4], (N_DP * CAP, D), jnp.float32) ** steps_of(splits[4], (N_DP * CAP, D), ((0, 256),), -0.2, 0.2)), 1.6954210479980247e-07, 1.6954210195763153e-06)
    return {"gradients": gradients, "owned_rows": owned_rows, "master": master, "first_moment": first_moment, "second_moment": second_moment}


beta_one = 0.9
beta_two = 0.999
adam_eps = 1e-08
learn_rate = 0.001
decay_rate = 0.1
clip_norm = 1.0

def slot_layout(owned_rows):
    row_starts = (jnp.cumsum(owned_rows) - owned_rows).astype(jnp.int32)
    slot_list = jnp.arange(N_DP * CAP, dtype=jnp.int32)
    owner_of = slot_list // CAP
    within_slot = slot_list % CAP
    live_mask = within_slot < owned_rows[owner_of]
    flat_rows = jnp.where(live_mask, row_starts[owner_of] + within_slot, 0).astype(jnp.int32)
    return (row_starts, flat_rows, live_mask)

def reference(gradients, owned_rows, master, first_moment, second_moment):

    def accumulate(running, replica_grad):
        return (running + replica_grad.astype(jnp.float32), None)
    summed, _ = lax.scan(accumulate, jnp.zeros((ROWS, D), jnp.float32), gradients)
    norm_sq = jnp.sum(summed * summed)
    clip_scale = jnp.minimum(1.0, clip_norm / (jnp.sqrt(norm_sq) + 1e-06))
    row_starts, flat_rows, live_mask = slot_layout(owned_rows)
    live_rows = live_mask[:, None]
    slot_grad = jnp.where(live_rows, summed[flat_rows], 0.0) * clip_scale
    new_first = beta_one * first_moment + (1.0 - beta_one) * slot_grad
    new_second = beta_two * second_moment + (1.0 - beta_two) * slot_grad * slot_grad
    first_hat = new_first / (1.0 - beta_one ** STEP)
    second_hat = new_second / (1.0 - beta_two ** STEP)
    direction = first_hat / (jnp.sqrt(second_hat) + adam_eps) + decay_rate * master
    new_master = master - learn_rate * direction
    new_master = jnp.where(live_rows, new_master, 0.0)
    new_first = jnp.where(live_rows, new_first, 0.0)
    new_second = jnp.where(live_rows, new_second, 0.0)
    direction = jnp.where(live_rows, direction, 0.0)
    slot_weights = new_master.astype(jnp.bfloat16)
    row_list = jnp.arange(ROWS, dtype=jnp.int32)
    row_owner = (lax.optimization_barrier(jnp.sum((row_starts[None, :] <= row_list[:, None]).astype(jnp.int32), axis=1)) - 1).astype(jnp.int32)
    row_slot = (row_owner * CAP + row_list - row_starts[row_owner]).astype(jnp.int32)
    weights = slot_weights[row_slot]
    return (new_master, new_first, new_second, direction, weights)
```

```python
import jax
import jax.numpy as jnp
from jax import lax
from jax.experimental import pallas as pl
from jax.experimental.pallas import tpu as pltpu
from jax.sharding import PartitionSpec as P

CAP = 3
STEP = 100

beta_one = 0.9
beta_two = 0.999
adam_eps = 1e-08
learn_rate = 0.001
decay_rate = 0.1
clip_norm = 1.0

ROWS = 384
WIDTH = 4608
HALF_TILES = 18
CHUNK = 640
SLOTS = 1024
ORDER = (2, 1, 3, 0)
OWN_TILES = (4, 5, 4, 5)

MESH = pl.DeviceIdType.MESH
f32 = jnp.float32
bf16 = jnp.bfloat16


def window_start(k):
    return (9 * k) // 2


def kernel(
    grad,
    owned,
    master,
    first,
    second,
    new_master,
    new_first,
    new_second,
    direction,
    weights,
    out_buf,
    own_buf,
    pair_buf,
    p_far,
    p_dir,
    p_mid,
    p_com,
    base,
    put,
    take,
    slot_buf,
    q_far,
    q_dir,
    q_mid,
    q_com,
    z_own,
    z_got,
    done_buf,
    norm_one,
    norm_two,
    norm_own,
    norm_mid,
    mine,
    grad_buf,
    w_full,
    w_send,
    w_got,
    e_all,
    flat_own,
    flat_pair,
    load_sem,
    pair_send,
    pair_recv,
    p_send,
    p_recv,
    q_send,
    q_recv,
    z_send,
    z_recv,
    t_send,
    t_recv,
    n1_send,
    n1_recv,
    n2_send,
    n2_recv,
    u_send,
    u_recv,
    zg_send,
    zg_recv,
    qg_send,
    qg_recv,
    pg_send,
    pg_recv,
    c_send,
    c_recv,
    out_sem,
):
    me = lax.axis_index("dp")
    y, x, z, c = me // 64, (me // 16) % 4, (me // 2) % 8, me % 2
    p = x + c * (y - x)
    q = y + c * (x - y)
    p_step = 16 + 48 * c
    q_step = 64 - 48 * c
    line, plane = me % 16, me // 16
    other = me + 1 - 2 * c

    def at_p(v):
        return me + (v - p) * p_step

    def at_q(v):
        return me + (v - q) * q_step

    def at_line(v):
        return me - line + v

    def at_plane(v):
        return v * 16 + line

    sends = []

    def send(src, dst, ssem, rsem, dev):
        copy = pltpu.make_async_remote_copy(
            src_ref=src, dst_ref=dst, send_sem=ssem, recv_sem=rsem,
            device_id=(dev,), device_id_type=MESH,
        )
        copy.start()
        sends.append(copy)

    def got(dst, ssem, rsem):
        pltpu.make_async_remote_copy(
            src_ref=dst, dst_ref=dst, send_sem=ssem, recv_sem=rsem,
            device_id=(other,), device_id_type=MESH,
        ).wait_recv()

    def columns(color, k):
        start = pl.multiple_of((HALF_TILES * color + window_start(k)) * 128, 128)
        return pl.ds(start, CHUNK)

    loads = {}
    for n, j in enumerate(ORDER):
        loads["out", j] = pltpu.make_async_copy(
            grad.at[0, :, columns(1 - c, (q + j) % 4)], out_buf.at[j], load_sem.at[n])
        loads["own", j] = pltpu.make_async_copy(
            grad.at[0, :, columns(c, (p + j) % 4)], own_buf.at[j], load_sem.at[4 + n])
    for j in ORDER:
        loads["out", j].start()
    for j in ORDER:
        loads["own", j].start()

    barrier = pltpu.get_barrier_semaphore()
    peers = [at_line((line + d) % 16) for d in range(1, 16)]
    peers += [at_plane((plane + d) % 16) for d in range(1, 16)]
    peers += [at_p((p + d) % 4) + 1 - 2 * c for d in range(1, 4)]
    peers += [at_q((q + d) % 4) + 1 - 2 * c for d in range(1, 4)]
    for dev in peers:
        pl.semaphore_signal(barrier, inc=1, device_id=(dev,), device_id_type=MESH)
    pl.semaphore_wait(barrier, len(peers))

    for j in ORDER:
        loads["out", j].wait()
        send(out_buf.at[j], pair_buf.at[j], pair_send.at[j], pair_recv.at[j], other)

    counts = owned[...].astype(f32)

    def owner_of(s):
        qq, zz, pp, cc = s // 256, (s // 32) % 8, (s // 8) % 4, (s // 4) % 2
        yy = qq + c * (pp - qq)
        xx = pp + c * (qq - pp)
        return yy * 64 + xx * 16 + zz * 2 + cc

    def put_step(i, carry):
        s = i * 128 + lax.broadcasted_iota(jnp.int32, (128, 256), 0)
        owner = owner_of(s)
        lane = lax.broadcasted_iota(jnp.int32, (128, 256), 1)
        count = jnp.sum(jnp.where(lane == owner, counts, 0.0), axis=1, keepdims=True)
        start = jnp.sum(jnp.where(lane < owner, counts, 0.0), axis=1, keepdims=True)
        slot = (lax.broadcasted_iota(jnp.int32, (128, 1), 0) % 4).astype(f32)
        row = jnp.where(slot < count, start + slot, -1.0)
        flat = lax.broadcasted_iota(jnp.int32, (128, ROWS), 1).astype(f32)
        put[pl.ds(pl.multiple_of(i * 128, 128), 128), :] = jnp.where(row == flat, 1.0, 0.0).astype(bf16)
        return carry

    lax.fori_loop(0, SLOTS // 128, put_step, 0)

    for i in range(4):
        s = i * 256 + lax.broadcasted_iota(jnp.int32, (256, 256), 1)
        owner = owner_of(s)
        holder = lax.broadcasted_iota(jnp.int32, (256, 256), 0)
        same = jnp.where(holder == owner, 1.0, 0.0).astype(bf16)
        earlier = jnp.where(holder < owner, 1.0, 0.0).astype(bf16)
        lhs = jnp.broadcast_to(counts, (8, 256)).astype(bf16)
        count = jnp.dot(lhs, same, preferred_element_type=f32)[0:1]
        start = jnp.dot(lhs, earlier, preferred_element_type=f32)[0:1]
        slot = (lax.broadcasted_iota(jnp.int32, (1, 256), 1) % 4).astype(f32)
        row = jnp.where(slot < count, start + slot, -1.0)
        flat = lax.broadcasted_iota(jnp.int32, (ROWS, 256), 0).astype(f32)
        take[:, i * 256:(i + 1) * 256] = jnp.where(row == flat, 1.0, 0.0).astype(bf16)

    def rows_add(dst, dst_at, terms, count, step=32):
        def body(i, carry):
            total = None
            for ref, at in terms:
                part = ref[pl.ds(pl.multiple_of(at + i * step, step), step), :].astype(f32)
                total = part if total is None else total + part
            dst[pl.ds(pl.multiple_of(dst_at + i * step, step), step), :] = total.astype(dst.dtype)
            return carry
        lax.fori_loop(0, count // step, body, 0)

    def ring_reduce(acc, half, prepare, far, direct, mid, com, ssem, rsem, nxt, prv, finish):
        lo, hi = pl.ds(0, half), pl.ds(half, half)
        prepare(2)
        send(acc.at[2, lo], far.at[0], ssem.at[0], rsem.at[0], nxt)
        send(acc.at[2, hi], far.at[1], ssem.at[1], rsem.at[1], prv)
        prepare(1)
        send(acc.at[1, hi], direct.at[1], ssem.at[2], rsem.at[2], nxt)
        prepare(3)
        send(acc.at[3, lo], direct.at[0], ssem.at[3], rsem.at[3], prv)
        prepare(0)
        got(far.at[0], ssem.at[0], rsem.at[0])
        rows_add(mid.at[0], 0, [(acc.at[1], 0), (far.at[0], 0)], half)
        send(mid.at[0], com.at[0], ssem.at[4], rsem.at[4], nxt)
        got(far.at[1], ssem.at[1], rsem.at[1])
        rows_add(mid.at[1], 0, [(acc.at[3], half), (far.at[1], 0)], half)
        send(mid.at[1], com.at[1], ssem.at[5], rsem.at[5], prv)
        got(direct.at[0], ssem.at[3], rsem.at[3])
        got(direct.at[1], ssem.at[2], rsem.at[2])
        got(com.at[0], ssem.at[4], rsem.at[4])
        rows_add(finish, 0, [(acc.at[0], 0), (direct.at[0], 0), (com.at[0], 0)], half)
        got(com.at[1], ssem.at[5], rsem.at[5])
        rows_add(finish, half, [(acc.at[0], half), (direct.at[1], 0), (com.at[1], 0)], half)

    def pair_prepare(j):
        loads["own", j].wait()
        got(pair_buf.at[j], pair_send.at[j], pair_recv.at[j])
        rows_add(own_buf.at[j], 0, [(own_buf.at[j], 0), (pair_buf.at[j], 0)], ROWS)

    ring_reduce(own_buf, 192, pair_prepare, p_far, p_dir, p_mid, p_com, p_send, p_recv,
                at_p((p + 1) % 4), at_p((p + 3) % 4), base)

    def slot_prepare(j):
        at = ((q + j) % 4) * 256
        def body(i, carry):
            rows = put[pl.ds(pl.multiple_of(at + i * 128, 128), 128), :]
            picked = jnp.dot(rows, base[...], preferred_element_type=f32)
            slot_buf[j, pl.ds(pl.multiple_of(i * 128, 128), 128), :] = picked.astype(bf16)
            return carry
        lax.fori_loop(0, 2, body, 0)

    ring_reduce(slot_buf, 128, slot_prepare, q_far, q_dir, q_mid, q_com, q_send, q_recv,
                at_q((q + 1) % 4), at_q((q + 3) % 4), z_own)

    for d in range(1, 8):
        to = (z + d) % 8
        send(z_own.at[pl.ds(pl.multiple_of(to * 32, 32), 32)], z_got.at[d],
             z_send.at[d], z_recv.at[d], me + (to - z) * 2)
    total = z_own[pl.ds(pl.multiple_of(z * 32, 32), 32), :].astype(f32)
    for d in range(1, 8):
        got(z_got.at[d], z_send.at[d], z_recv.at[d])
        total = total + z_got[d].astype(f32)
    for k in range(4):
        done_buf[k] = total[8 * k:8 * k + 8]

    fifth = (p % 2).astype(f32)
    squares = total * total
    squares = squares[0:8] + squares[8:16] + squares[16:24] + squares[24:32]
    part = squares[:, 512:640] * fifth
    for k in range(4):
        part = part + squares[:, 128 * k:128 * k + 128]
    norm_own[...] = part
    for d in range(1, 16):
        send(norm_own, norm_one.at[d], n1_send.at[d], n1_recv.at[d], at_line((line + d) % 16))

    for core in range(2):
        for d in range(4):
            to = (p + d) % 4
            n = core * 4 + d
            dev = at_p(to) + core - c
            if d == 0:
                @pl.when(c != core)
                def _():
                    pltpu.make_async_remote_copy(
                        src_ref=done_buf.at[p], dst_ref=mine.at[c, p],
                        send_sem=t_send.at[n], recv_sem=t_recv.at[c, d],
                        device_id=(dev,), device_id_type=MESH).start()
            else:
                send(done_buf.at[to], mine.at[c, p], t_send.at[n], t_recv.at[c, d], dev)
    mine[c, p] = done_buf[p]

    for d in range(1, 16):
        got(norm_one.at[d], n1_send.at[d], n1_recv.at[d])
        part = part + norm_one[d]
    norm_mid[...] = part
    for d in range(1, 16):
        send(norm_mid, norm_two.at[d], n2_send.at[d], n2_recv.at[d], at_plane((plane + d) % 16))

    for color in range(2):
        for d in range(4):
            def wait(color=color, d=d):
                got(mine.at[0, 0], t_send.at[0], t_recv.at[color, d])
            if d == 0:
                pl.when(c != color)(wait)
            else:
                wait()
    for color in range(2):
        for k in range(4):
            at = (HALF_TILES * color + window_start(k)) * 128
            width = OWN_TILES[k] * 128
            grad_buf[:, at:at + width] = mine[color, k, :, 0:width]
    own_grad = jnp.where(c == 0, grad_buf[0:3, :], grad_buf[4:7, :])

    for d in range(1, 16):
        got(norm_two.at[d], n2_send.at[d], n2_recv.at[d])
        part = part + norm_two[d]
    norm_sq = jnp.sum(jnp.sum(part, axis=1, keepdims=True), axis=0, keepdims=True)
    clip_scale = jnp.minimum(1.0, clip_norm / (jnp.sqrt(norm_sq) + 1e-06))

    holders = lax.broadcasted_iota(jnp.int32, (1, 256), 1)
    my_count = jnp.sum(jnp.where(holders == me, counts, 0.0), axis=1, keepdims=True)
    live = lax.broadcasted_iota(jnp.int32, (3, WIDTH), 0).astype(f32) < my_count
    slot_grad = jnp.where(live, own_grad, 0.0) * clip_scale
    m = beta_one * first[...] + (1.0 - beta_one) * slot_grad
    v = beta_two * second[...] + (1.0 - beta_two) * slot_grad * slot_grad
    first_hat = m / (1.0 - beta_one**STEP)
    second_hat = v / (1.0 - beta_two**STEP)
    step = first_hat / (jnp.sqrt(second_hat) + adam_eps) + decay_rate * master[...]
    w = master[...] - learn_rate * step
    w = jnp.where(live, w, 0.0)
    new_master[...] = w
    new_first[...] = jnp.where(live, m, 0.0)
    new_second[...] = jnp.where(live, v, 0.0)
    direction[...] = jnp.where(live, step, 0.0)

    w_full[...] = jnp.zeros_like(w_full)

    @pl.when(c == 0)
    def _():
        w_full[0:3, :] = w

    @pl.when(c == 1)
    def _():
        w_full[4:7, :] = w

    for color in range(2):
        for k in range(4):
            at = (HALF_TILES * color + window_start(k)) * 128
            w_send[color, k] = w_full[:, at:at + CHUNK]
    for color in range(2):
        here = x if color == 0 else y
        stride = 16 if color == 0 else 64
        for d in range(4):
            to = (here + d) % 4
            n = color * 4 + d
            dev = me + (to - here) * stride + color - c
            if d == 0:
                @pl.when(c != color)
                def _():
                    pltpu.make_async_remote_copy(
                        src_ref=w_send.at[color, here], dst_ref=w_got.at[here, c],
                        send_sem=u_send.at[n], recv_sem=u_recv.at[c, d],
                        device_id=(dev,), device_id_type=MESH).start()
            else:
                send(w_send.at[color, to], w_got.at[here, c], u_send.at[n], u_recv.at[c, d], dev)
    w_got[p, c] = w_send[c, p]
    for core in range(2):
        for d in range(4):
            def wait(core=core, d=d):
                got(w_got.at[0, 0], u_send.at[0], u_recv.at[core, d])
            if d == 0:
                pl.when(c != core)(wait)
            else:
                wait()
    rows = jnp.concatenate([w_got[k, 0] + w_got[k, 1] for k in range(4)], axis=0)
    place = pl.multiple_of(q * 256 + z * 32, 32)
    e_all[pl.ds(place, 32), :] = rows.astype(bf16)

    for d in range(1, 8):
        to = (z + d) % 8
        send(e_all.at[pl.ds(place, 32)], e_all.at[pl.ds(place, 32)],
             zg_send.at[d], zg_recv.at[d], me + (to - z) * 2)
    for d in range(1, 8):
        came = pl.multiple_of(q * 256 + ((z + 8 - d) % 8) * 32, 32)
        got(e_all.at[pl.ds(came, 32)], zg_send.at[d], zg_recv.at[d])

    def ring_gather(part_of, pos, ssem, rsem, nxt, prv, after=None):
        def push(k, h, s, dev):
            send(part_of(k, h), part_of(k, h), ssem.at[s], rsem.at[s], dev)

        def come(k, h, s):
            got(part_of(k, h), ssem.at[s], rsem.at[s])

        push(pos, 0, 0, prv)
        push(pos, 1, 1, nxt)
        push(pos, 1, 2, prv)
        push(pos, 0, 3, nxt)
        if after is not None:
            after(pos)
        above, below, far = (pos + 1) % 4, (pos + 3) % 4, (pos + 2) % 4
        come(above, 0, 0)
        push(above, 0, 4, prv)
        come(below, 1, 1)
        push(below, 1, 5, nxt)
        come(above, 1, 2)
        if after is not None:
            after(above)
        come(below, 0, 3)
        if after is not None:
            after(below)
        come(far, 0, 4)
        come(far, 1, 5)
        if after is not None:
            after(far)

    ring_gather(lambda k, h: e_all.at[pl.ds(pl.multiple_of(k * 256 + h * 128, 128), 128)],
                q, qg_send, qg_recv, at_q((q + 1) % 4), at_q((q + 3) % 4))

    def take_step(i, carry):
        at = pl.multiple_of(i * 128, 128)
        picked = jnp.dot(take[pl.ds(at, 128), :], e_all[...], preferred_element_type=f32)
        flat_own[p, pl.ds(at, 128), :] = picked.astype(bf16)
        return carry

    lax.fori_loop(0, 3, take_step, 0)

    order = []

    def pass_on(k):
        n = len(order)
        order.append(k)
        send(flat_own.at[k], flat_pair.at[k], c_send.at[n], c_recv.at[n], other)

    ring_gather(lambda k, h: flat_own.at[k, pl.ds(h * 192, 192)],
                p, pg_send, pg_recv, at_p((p + 1) % 4), at_p((p + 3) % 4), pass_on)
    stores = []

    def store(buf, color, k, n):
        at = pl.multiple_of((HALF_TILES * color + window_start(k)) * 128, 128)
        width = OWN_TILES[k] * 128
        copy = pltpu.make_async_copy(
            buf.at[k, :, pl.ds(0, width)], weights.at[:, pl.ds(at, width)], out_sem.at[n])
        copy.start()
        stores.append(copy)

    for k in range(4):
        store(flat_own, c, k, k)
    for n, d in enumerate((0, 1, 3, 2)):
        got(flat_pair.at[(q + d) % 4], c_send.at[n], c_recv.at[n])
    for k in range(4):
        store(flat_pair, 1 - c, k, 4 + k)

    for copy in stores:
        copy.wait()
    for copy in sends:
        copy.wait_send()
    for core in range(2):
        @pl.when(c != core)
        def _():
            pltpu.make_async_remote_copy(
                src_ref=done_buf.at[0], dst_ref=mine.at[0, 0],
                send_sem=t_send.at[core * 4], recv_sem=t_recv.at[0, 0],
                device_id=(other,), device_id_type=MESH).wait_send()
            pltpu.make_async_remote_copy(
                src_ref=w_send.at[0, 0], dst_ref=w_got.at[0, 0],
                send_sem=u_send.at[core * 4], recv_sem=u_recv.at[0, 0],
                device_id=(other,), device_id_type=MESH).wait_send()


def per_device(gradients, owned_rows, master, first_moment, second_moment):
    vmem = pl.BlockSpec(memory_space=pltpu.VMEM)
    hbm = pl.BlockSpec(memory_space=pl.ANY)
    state = jax.ShapeDtypeStruct(master.shape, f32)
    dma = pltpu.SemaphoreType.DMA
    return pl.pallas_call(
        kernel,
        out_shape=(state, state, state, state, jax.ShapeDtypeStruct((ROWS, WIDTH), bf16)),
        in_specs=[hbm, vmem, vmem, vmem, vmem],
        out_specs=(vmem, vmem, vmem, vmem, hbm),
        scratch_shapes=[
            pltpu.VMEM((4, ROWS, CHUNK), bf16),
            pltpu.VMEM((4, ROWS, CHUNK), bf16),
            pltpu.VMEM((4, ROWS, CHUNK), bf16),
            pltpu.VMEM((2, 192, CHUNK), bf16),
            pltpu.VMEM((2, 192, CHUNK), bf16),
            pltpu.VMEM((2, 192, CHUNK), bf16),
            pltpu.VMEM((2, 192, CHUNK), bf16),
            pltpu.VMEM((ROWS, CHUNK), bf16),
            pltpu.VMEM((SLOTS, ROWS), bf16),
            pltpu.VMEM((ROWS, SLOTS), bf16),
            pltpu.VMEM((4, 256, CHUNK), bf16),
            pltpu.VMEM((2, 128, CHUNK), bf16),
            pltpu.VMEM((2, 128, CHUNK), bf16),
            pltpu.VMEM((2, 128, CHUNK), bf16),
            pltpu.VMEM((2, 128, CHUNK), bf16),
            pltpu.VMEM((256, CHUNK), bf16),
            pltpu.VMEM((8, 32, CHUNK), bf16),
            pltpu.VMEM((4, 8, CHUNK), f32),
            pltpu.VMEM((16, 8, 128), f32),
            pltpu.VMEM((16, 8, 128), f32),
            pltpu.VMEM((8, 128), f32),
            pltpu.VMEM((8, 128), f32),
            pltpu.VMEM((2, 4, 8, CHUNK), f32),
            pltpu.VMEM((8, WIDTH), f32),
            pltpu.VMEM((8, WIDTH), f32),
            pltpu.VMEM((2, 4, 8, CHUNK), f32),
            pltpu.VMEM((4, 2, 8, CHUNK), f32),
            pltpu.VMEM((SLOTS, CHUNK), bf16),
            pltpu.VMEM((4, ROWS, CHUNK), bf16),
            pltpu.VMEM((4, ROWS, CHUNK), bf16),
            dma((8,)),
            dma((4,)), dma((4,)),
            dma((6,)), dma((6,)),
            dma((6,)), dma((6,)),
            dma((8,)), dma((8,)),
            dma((8,)), dma((2, 4)),
            dma((16,)), dma((16,)),
            dma((16,)), dma((16,)),
            dma((8,)), dma((2, 4)),
            dma((8,)), dma((8,)),
            dma((6,)), dma((6,)),
            dma((6,)), dma((6,)),
            dma((4,)), dma((4,)),
            dma((8,)),
        ],
        compiler_params=pltpu.CompilerParams(
            collective_id=0, has_side_effects=True, vmem_limit_bytes=48 * 1024 * 1024),
    )(gradients, owned_rows.reshape(1, -1), master, first_moment, second_moment)


def solution(mesh):
    in_specs = (P("dp", None, None), P(), P("dp", None), P("dp", None), P("dp", None))
    out_specs = (P("dp", None), P("dp", None), P("dp", None), P("dp", None), P())
    return jax.shard_map(
        per_device, mesh=mesh, in_specs=in_specs, out_specs=out_specs, check_vma=False
    )
```

```python
import jax
import jax.numpy as jnp
from jax import lax
from jax.experimental import pallas as pl
from jax.experimental.pallas import tpu as pltpu
from jax.sharding import PartitionSpec as P

CAP = 3
STEP = 100

beta_one = 0.9
beta_two = 0.999
adam_eps = 1e-08
learn_rate = 0.001
decay_rate = 0.1
clip_norm = 1.0

ROWS = 384
WIDTH = 4608
HALF_TILES = 18
CHUNK = 640
SLOTS = 1024
ORDER = (2, 1, 3, 0)
OWN_TILES = (4, 5, 4, 5)

MESH = pl.DeviceIdType.MESH
f32 = jnp.float32
bf16 = jnp.bfloat16


def window_start(k):
    return (9 * k) // 2


def kernel(
    grad,
    owned_hbm,
    master_hbm,
    first_hbm,
    second_hbm,
    new_master,
    new_first,
    new_second,
    direction,
    flat_own,
    flat_pair,
    owned,
    master,
    first,
    second,
    out_buf,
    own_buf,
    pair_buf,
    p_far,
    p_dir,
    p_mid,
    p_com,
    base,
    put,
    take,
    slot_buf,
    q_far,
    q_dir,
    q_mid,
    q_com,
    z_own,
    z_got,
    done_buf,
    norm_one,
    norm_two,
    norm_own,
    norm_mid,
    mine,
    grad_buf,
    s_full,
    s_send,
    s_got,
    e_all,
    load_sem,
    pair_send,
    pair_recv,
    p_send,
    p_recv,
    q_send,
    q_recv,
    z_send,
    z_recv,
    t_send,
    t_recv,
    n1_send,
    n1_recv,
    n2_send,
    n2_recv,
    u_send,
    u_recv,
    zg_send,
    zg_recv,
    qg_send,
    qg_recv,
    pg_send,
    pg_recv,
    c_send,
    c_recv,
):
    me = lax.axis_index("dp")
    y, x, z, c = me // 64, (me // 16) % 4, (me // 2) % 8, me % 2
    p = x + c * (y - x)
    q = y + c * (x - y)
    p_step = 16 + 48 * c
    q_step = 64 - 48 * c
    line, plane = me % 16, me // 16
    other = me + 1 - 2 * c

    def at_p(v):
        return me + (v - p) * p_step

    def at_q(v):
        return me + (v - q) * q_step

    def at_line(v):
        return me - line + v

    def at_plane(v):
        return v * 16 + line

    sends = []

    def send(src, dst, ssem, rsem, dev):
        copy = pltpu.make_async_remote_copy(
            src_ref=src, dst_ref=dst, send_sem=ssem, recv_sem=rsem,
            device_id=(dev,), device_id_type=MESH,
        )
        copy.start()
        sends.append(copy)

    def got(dst, ssem, rsem):
        pltpu.make_async_remote_copy(
            src_ref=dst, dst_ref=dst, send_sem=ssem, recv_sem=rsem,
            device_id=(other,), device_id_type=MESH,
        ).wait_recv()

    def columns(color, k):
        start = pl.multiple_of((HALF_TILES * color + window_start(k)) * 128, 128)
        return pl.ds(start, CHUNK)

    loads = {}
    for n, j in enumerate(ORDER):
        loads["out", j] = pltpu.make_async_copy(
            grad.at[0, :, columns(1 - c, (q + j) % 4)], out_buf.at[j], load_sem.at[n])
        loads["own", j] = pltpu.make_async_copy(
            grad.at[0, :, columns(c, (p + j) % 4)], own_buf.at[j], load_sem.at[4 + n])
    small = [
        pltpu.make_async_copy(src, dst, load_sem.at[8 + n])
        for n, (src, dst) in enumerate(
            ((owned_hbm, owned), (master_hbm, master), (first_hbm, first), (second_hbm, second)))
    ]
    for copy in small:
        copy.start()
    for j in ORDER:
        loads["out", j].start()
    for j in ORDER:
        loads["own", j].start()

    barrier = pltpu.get_barrier_semaphore()
    peers = [at_line((line + d) % 16) for d in range(1, 16)]
    peers += [at_plane((plane + d) % 16) for d in range(1, 16)]
    peers += [at_p((p + d) % 4) + 1 - 2 * c for d in range(1, 4)]
    peers += [at_q((q + d) % 4) + 1 - 2 * c for d in range(1, 4)]
    for dev in peers:
        pl.semaphore_signal(barrier, inc=1, device_id=(dev,), device_id_type=MESH)
    for copy in small:
        copy.wait()
    counts = owned[...].astype(f32)

    def owner_of(s):
        qq, zz, pp, cc = s // 256, (s // 32) % 8, (s // 8) % 4, (s // 4) % 2
        yy = qq + c * (pp - qq)
        xx = pp + c * (qq - pp)
        return yy * 64 + xx * 16 + zz * 2 + cc

    def put_step(i, carry):
        s = i * 128 + lax.broadcasted_iota(jnp.int32, (128, 256), 0)
        owner = owner_of(s)
        lane = lax.broadcasted_iota(jnp.int32, (128, 256), 1)
        count = jnp.sum(jnp.where(lane == owner, counts, 0.0), axis=1, keepdims=True)
        start = jnp.sum(jnp.where(lane < owner, counts, 0.0), axis=1, keepdims=True)
        slot = (lax.broadcasted_iota(jnp.int32, (128, 1), 0) % 4).astype(f32)
        row = jnp.where(slot < count, start + slot, -1.0)
        flat = lax.broadcasted_iota(jnp.int32, (128, ROWS), 1).astype(f32)
        put[pl.ds(pl.multiple_of(i * 128, 128), 128), :] = jnp.where(row == flat, 1.0, 0.0).astype(bf16)
        return carry

    lax.fori_loop(0, SLOTS // 128, put_step, 0)

    for i in range(4):
        s = i * 256 + lax.broadcasted_iota(jnp.int32, (256, 256), 1)
        owner = owner_of(s)
        holder = lax.broadcasted_iota(jnp.int32, (256, 256), 0)
        same = jnp.where(holder == owner, 1.0, 0.0).astype(bf16)
        earlier = jnp.where(holder < owner, 1.0, 0.0).astype(bf16)
        lhs = jnp.broadcast_to(counts, (8, 256)).astype(bf16)
        count = jnp.dot(lhs, same, preferred_element_type=f32)[0:1]
        start = jnp.dot(lhs, earlier, preferred_element_type=f32)[0:1]
        slot = (lax.broadcasted_iota(jnp.int32, (1, 256), 1) % 4).astype(f32)
        row = jnp.where(slot < count, start + slot, -1.0)
        flat = lax.broadcasted_iota(jnp.int32, (ROWS, 256), 0).astype(f32)
        take[:, i * 256:(i + 1) * 256] = jnp.where(row == flat, 1.0, 0.0).astype(bf16)

    s_full[...] = jnp.zeros_like(s_full)
    for core in range(2):
        @pl.when(c == core)
        def _():
            for a, ref in enumerate((master, first, second)):
                s_full[8 * a + 4 * core:8 * a + 4 * core + 3, :] = ref[...]
    for color in range(2):
        for k in range(4):
            at = (HALF_TILES * color + window_start(k)) * 128
            s_send[color, k] = s_full[:, at:at + CHUNK]

    pl.semaphore_wait(barrier, len(peers))

    for j in ORDER:
        loads["out", j].wait()
        send(out_buf.at[j], pair_buf.at[j], pair_send.at[j], pair_recv.at[j], other)

    def rows_add(dst, dst_at, terms, count, step=32):
        def body(i, carry):
            total = None
            for ref, at in terms:
                part = ref[pl.ds(pl.multiple_of(at + i * step, step), step), :].astype(f32)
                total = part if total is None else total + part
            dst[pl.ds(pl.multiple_of(dst_at + i * step, step), step), :] = total.astype(dst.dtype)
            return carry
        lax.fori_loop(0, count // step, body, 0)

    def ring_reduce(acc, half, prepare, far, direct, mid, com, ssem, rsem, nxt, prv, finish):
        part = half // 2
        prepare(2)
        for n in range(2):
            piece = pl.ds(n * part, part)
            send(acc.at[2, piece], far.at[0, piece], ssem.at[n], rsem.at[n], nxt)
            send(acc.at[2, pl.ds(half + n * part, part)], far.at[1, piece], ssem.at[2 + n], rsem.at[2 + n], prv)
        prepare(1)
        send(acc.at[1, pl.ds(half, half)], direct.at[1], ssem.at[4], rsem.at[4], nxt)
        prepare(3)
        send(acc.at[3, pl.ds(0, half)], direct.at[0], ssem.at[5], rsem.at[5], prv)
        prepare(0)
        for n in range(2):
            piece = pl.ds(n * part, part)
            got(far.at[0, piece], ssem.at[n], rsem.at[n])
            rows_add(mid.at[0], n * part, [(acc.at[1], n * part), (far.at[0], n * part)], part)
            send(mid.at[0, piece], com.at[0, piece], ssem.at[6 + n], rsem.at[6 + n], nxt)
            got(far.at[1, piece], ssem.at[2 + n], rsem.at[2 + n])
            rows_add(mid.at[1], n * part, [(acc.at[3], half + n * part), (far.at[1], n * part)], part)
            send(mid.at[1, piece], com.at[1, piece], ssem.at[8 + n], rsem.at[8 + n], prv)
        got(direct.at[0], ssem.at[5], rsem.at[5])
        got(direct.at[1], ssem.at[4], rsem.at[4])
        for n in range(2):
            piece = pl.ds(n * part, part)
            got(com.at[0, piece], ssem.at[6 + n], rsem.at[6 + n])
            rows_add(finish, n * part, [(acc.at[0], n * part), (direct.at[0], n * part), (com.at[0], n * part)], part)
            got(com.at[1, piece], ssem.at[8 + n], rsem.at[8 + n])
            rows_add(finish, half + n * part, [(acc.at[0], half + n * part), (direct.at[1], n * part), (com.at[1], n * part)], part)

    def pair_prepare(j):
        loads["own", j].wait()
        got(pair_buf.at[j], pair_send.at[j], pair_recv.at[j])
        rows_add(own_buf.at[j], 0, [(own_buf.at[j], 0), (pair_buf.at[j], 0)], ROWS)

    ring_reduce(own_buf, 192, pair_prepare, p_far, p_dir, p_mid, p_com, p_send, p_recv,
                at_p((p + 1) % 4), at_p((p + 3) % 4), base)

    def slot_prepare(j):
        at = ((q + j) % 4) * 256
        def body(i, carry):
            rows = put[pl.ds(pl.multiple_of(at + i * 128, 128), 128), :]
            picked = jnp.dot(rows, base[...], preferred_element_type=f32)
            slot_buf[j, pl.ds(pl.multiple_of(i * 128, 128), 128), :] = picked.astype(bf16)
            return carry
        lax.fori_loop(0, 2, body, 0)

    ring_reduce(slot_buf, 128, slot_prepare, q_far, q_dir, q_mid, q_com, q_send, q_recv,
                at_q((q + 1) % 4), at_q((q + 3) % 4), z_own)

    for d in range(1, 8):
        to = (z + d) % 8
        send(z_own.at[pl.ds(pl.multiple_of(to * 32, 32), 32)], z_got.at[d],
             z_send.at[d], z_recv.at[d], me + (to - z) * 2)

    for color in range(2):
        here = x if color == 0 else y
        stride = 16 if color == 0 else 64
        for d in range(4):
            to = (here + d) % 4
            n = color * 4 + d
            dev = me + (to - here) * stride + color - c
            if d == 0:
                @pl.when(c != color)
                def _():
                    pltpu.make_async_remote_copy(
                        src_ref=s_send.at[color, here], dst_ref=s_got.at[here, c],
                        send_sem=u_send.at[n], recv_sem=u_recv.at[c, d],
                        device_id=(dev,), device_id_type=MESH).start()
            else:
                send(s_send.at[color, to], s_got.at[here, c], u_send.at[n], u_recv.at[c, d], dev)
    s_got[p, c] = s_send[c, p]

    total = z_own[pl.ds(pl.multiple_of(z * 32, 32), 32), :].astype(f32)
    for d in range(1, 8):
        got(z_got.at[d], z_send.at[d], z_recv.at[d])
        total = total + z_got[d].astype(f32)
    for k in range(4):
        done_buf[k] = total[8 * k:8 * k + 8]

    fifth = (p % 2).astype(f32)
    squares = total * total
    squares = squares[0:8] + squares[8:16] + squares[16:24] + squares[24:32]
    part = squares[:, 512:640] * fifth
    for k in range(4):
        part = part + squares[:, 128 * k:128 * k + 128]
    norm_own[...] = part
    for d in range(1, 16):
        send(norm_own, norm_one.at[d], n1_send.at[d], n1_recv.at[d], at_line((line + d) % 16))

    for core in range(2):
        for d in range(4):
            to = (p + d) % 4
            n = core * 4 + d
            dev = at_p(to) + core - c
            if d == 0:
                @pl.when(c != core)
                def _():
                    pltpu.make_async_remote_copy(
                        src_ref=done_buf.at[p], dst_ref=mine.at[c, p],
                        send_sem=t_send.at[n], recv_sem=t_recv.at[c, d],
                        device_id=(dev,), device_id_type=MESH).start()
            else:
                send(done_buf.at[to], mine.at[c, p], t_send.at[n], t_recv.at[c, d], dev)
    mine[c, p] = done_buf[p]

    for d in range(1, 16):
        got(norm_one.at[d], n1_send.at[d], n1_recv.at[d])
        part = part + norm_one[d]
    norm_mid[...] = part
    for d in range(1, 16):
        send(norm_mid, norm_two.at[d], n2_send.at[d], n2_recv.at[d], at_plane((plane + d) % 16))

    for core in range(2):
        for d in range(4):
            def wait(core=core, d=d):
                got(s_got.at[0, 0], u_send.at[0], u_recv.at[core, d])
            if d == 0:
                pl.when(c != core)(wait)
            else:
                wait()
    states = [
        jnp.concatenate([s_got[k, 0, 8 * a:8 * a + 8] + s_got[k, 1, 8 * a:8 * a + 8] for k in range(4)], axis=0)
        for a in range(3)
    ]

    for d in range(1, 16):
        got(norm_two.at[d], n2_send.at[d], n2_recv.at[d])
        part = part + norm_two[d]
    norm_sq = jnp.sum(jnp.sum(part, axis=1, keepdims=True), axis=0, keepdims=True)
    clip_scale = jnp.minimum(1.0, clip_norm / (jnp.sqrt(norm_sq) + 1e-06))

    def update(slot_grad, weight, moment, square):
        m = beta_one * moment + (1.0 - beta_one) * slot_grad
        v = beta_two * square + (1.0 - beta_two) * slot_grad * slot_grad
        first_hat = m / (1.0 - beta_one**STEP)
        second_hat = v / (1.0 - beta_two**STEP)
        step = first_hat / (jnp.sqrt(second_hat) + adam_eps) + decay_rate * weight
        return weight - learn_rate * step, m, v, step

    rows, _, _, _ = update(total * clip_scale, *states)
    place = pl.multiple_of(q * 256 + z * 32, 32)
    e_all[pl.ds(place, 32), :] = rows.astype(bf16)

    for d in range(1, 8):
        to = (z + d) % 8
        send(e_all.at[pl.ds(place, 32)], e_all.at[pl.ds(place, 32)],
             zg_send.at[d], zg_recv.at[d], me + (to - z) * 2)

    for color in range(2):
        for d in range(4):
            def wait(color=color, d=d):
                got(mine.at[0, 0], t_send.at[0], t_recv.at[color, d])
            if d == 0:
                pl.when(c != color)(wait)
            else:
                wait()
    for color in range(2):
        for k in range(4):
            at = (HALF_TILES * color + window_start(k)) * 128
            width = OWN_TILES[k] * 128
            grad_buf[:, at:at + width] = mine[color, k, :, 0:width]
    own_grad = jnp.where(c == 0, grad_buf[0:3, :], grad_buf[4:7, :])
    holders = lax.broadcasted_iota(jnp.int32, (1, 256), 1)
    my_count = jnp.sum(jnp.where(holders == me, counts, 0.0), axis=1, keepdims=True)
    live = lax.broadcasted_iota(jnp.int32, (3, WIDTH), 0).astype(f32) < my_count
    w, m, v, step = update(jnp.where(live, own_grad, 0.0) * clip_scale, master[...], first[...], second[...])
    new_master[...] = jnp.where(live, w, 0.0)
    new_first[...] = jnp.where(live, m, 0.0)
    new_second[...] = jnp.where(live, v, 0.0)
    direction[...] = jnp.where(live, step, 0.0)

    for d in range(1, 8):
        came = pl.multiple_of(q * 256 + ((z + 8 - d) % 8) * 32, 32)
        got(e_all.at[pl.ds(came, 32)], zg_send.at[d], zg_recv.at[d])

    def ring_gather(part_of, half, pos, ssem, rsem, nxt, prv, after=None):
        quarter = half // 2
        above, below, far = (pos + 1) % 4, (pos + 3) % 4, (pos + 2) % 4

        def push(k, at, size, s, dev):
            send(part_of(k, at, size), part_of(k, at, size), ssem.at[s], rsem.at[s], dev)

        def come(k, at, size, s):
            got(part_of(k, at, size), ssem.at[s], rsem.at[s])

        for n in range(2):
            push(pos, n * quarter, quarter, n, prv)
            push(pos, half + n * quarter, quarter, 2 + n, nxt)
        push(pos, half, half, 4, prv)
        push(pos, 0, half, 5, nxt)
        if after is not None:
            after(pos, 0, 2 * half)
        for n in range(2):
            come(above, n * quarter, quarter, n)
            push(above, n * quarter, quarter, 6 + n, prv)
            come(below, half + n * quarter, quarter, 2 + n)
            push(below, half + n * quarter, quarter, 8 + n, nxt)
        come(above, half, half, 4)
        if after is not None:
            after(above, 0, 2 * half)
        come(below, 0, half, 5)
        if after is not None:
            after(below, 0, 2 * half)
        for n in range(2):
            come(far, n * quarter, quarter, 6 + n)
            if after is not None:
                after(far, n * quarter, quarter)
            come(far, half + n * quarter, quarter, 8 + n)
            if after is not None:
                after(far, half + n * quarter, quarter)

    ring_gather(lambda k, at, size: e_all.at[pl.ds(pl.multiple_of(k * 256 + at, 64), size)],
                128, q, qg_send, qg_recv, at_q((q + 1) % 4), at_q((q + 3) % 4))

    def take_step(i, carry):
        at = pl.multiple_of(i * 128, 128)
        picked = jnp.dot(take[pl.ds(at, 128), :], e_all[...], preferred_element_type=f32)
        flat_own[p, pl.ds(at, 128), :] = picked.astype(bf16)
        return carry

    lax.fori_loop(0, 3, take_step, 0)

    passed = []

    def pass_on(k, at, size):
        n = len(passed)
        passed.append((at, size))
        rows = pl.ds(at, size)
        send(flat_own.at[k, rows], flat_pair.at[k, rows], c_send.at[n], c_recv.at[n], other)

    ring_gather(lambda k, at, size: flat_own.at[k, pl.ds(at, size)],
                192, p, pg_send, pg_recv, at_p((p + 1) % 4), at_p((p + 3) % 4), pass_on)
    for n, (at, size) in enumerate(passed):
        d = (0, 1, 3, 2, 2, 2, 2)[n]
        got(flat_pair.at[(q + d) % 4, pl.ds(at, size)], c_send.at[n], c_recv.at[n])

    for copy in sends:
        copy.wait_send()
    for core in range(2):
        @pl.when(c != core)
        def _():
            pltpu.make_async_remote_copy(
                src_ref=done_buf.at[0], dst_ref=mine.at[0, 0],
                send_sem=t_send.at[core * 4], recv_sem=t_recv.at[0, 0],
                device_id=(other,), device_id_type=MESH).wait_send()
            pltpu.make_async_remote_copy(
                src_ref=s_send.at[0, 0], dst_ref=s_got.at[0, 0],
                send_sem=u_send.at[core * 4], recv_sem=u_recv.at[0, 0],
                device_id=(other,), device_id_type=MESH).wait_send()


def write(new_master, new_first, new_second, direction, flat_own, flat_pair,
          master_out, first_out, second_out, direction_out, weights, sem):
    c = lax.axis_index("dp") % 2
    copies = [
        pltpu.make_async_copy(src, dst, sem.at[8 + n])
        for n, (src, dst) in enumerate(
            ((new_master, master_out), (new_first, first_out), (new_second, second_out), (direction, direction_out)))
    ]
    for n, (buf, color) in enumerate(((flat_own, c), (flat_pair, 1 - c))):
        for k in range(4):
            at = pl.multiple_of((HALF_TILES * color + window_start(k)) * 128, 128)
            width = OWN_TILES[k] * 128
            copies.append(pltpu.make_async_copy(
                buf.at[k, :, pl.ds(0, width)], weights.at[:, pl.ds(at, width)], sem.at[4 * n + k]))
    for copy in copies:
        copy.start()
    for copy in copies:
        copy.wait()


def per_device(gradients, owned_rows, master, first_moment, second_moment):
    vmem = pl.BlockSpec(memory_space=pltpu.VMEM)
    hbm = pl.BlockSpec(memory_space=pltpu.HBM)
    state = jax.ShapeDtypeStruct(master.shape, f32)
    flat = jax.ShapeDtypeStruct((4, ROWS, CHUNK), bf16)
    dma = pltpu.SemaphoreType.DMA
    results = pl.pallas_call(
        kernel,
        out_shape=(state, state, state, state, flat, flat),
        in_specs=[hbm] * 5,
        out_specs=(vmem,) * 6,
        scratch_shapes=[
            pltpu.VMEM((1, 256), jnp.int32),
            pltpu.VMEM(master.shape, f32),
            pltpu.VMEM(master.shape, f32),
            pltpu.VMEM(master.shape, f32),
            pltpu.VMEM((4, ROWS, CHUNK), bf16),
            pltpu.VMEM((4, ROWS, CHUNK), bf16),
            pltpu.VMEM((4, ROWS, CHUNK), bf16),
            pltpu.VMEM((2, 192, CHUNK), bf16),
            pltpu.VMEM((2, 192, CHUNK), bf16),
            pltpu.VMEM((2, 192, CHUNK), bf16),
            pltpu.VMEM((2, 192, CHUNK), bf16),
            pltpu.VMEM((ROWS, CHUNK), bf16),
            pltpu.VMEM((SLOTS, ROWS), bf16),
            pltpu.VMEM((ROWS, SLOTS), bf16),
            pltpu.VMEM((4, 256, CHUNK), bf16),
            pltpu.VMEM((2, 128, CHUNK), bf16),
            pltpu.VMEM((2, 128, CHUNK), bf16),
            pltpu.VMEM((2, 128, CHUNK), bf16),
            pltpu.VMEM((2, 128, CHUNK), bf16),
            pltpu.VMEM((256, CHUNK), bf16),
            pltpu.VMEM((8, 32, CHUNK), bf16),
            pltpu.VMEM((4, 8, CHUNK), f32),
            pltpu.VMEM((16, 8, 128), f32),
            pltpu.VMEM((16, 8, 128), f32),
            pltpu.VMEM((8, 128), f32),
            pltpu.VMEM((8, 128), f32),
            pltpu.VMEM((2, 4, 8, CHUNK), f32),
            pltpu.VMEM((8, WIDTH), f32),
            pltpu.VMEM((24, WIDTH), f32),
            pltpu.VMEM((2, 4, 24, CHUNK), f32),
            pltpu.VMEM((4, 2, 24, CHUNK), f32),
            pltpu.VMEM((SLOTS, CHUNK), bf16),
            dma((12,)),
            dma((4,)), dma((4,)),
            dma((10,)), dma((10,)),
            dma((10,)), dma((10,)),
            dma((8,)), dma((8,)),
            dma((8,)), dma((2, 4)),
            dma((16,)), dma((16,)),
            dma((16,)), dma((16,)),
            dma((8,)), dma((2, 4)),
            dma((8,)), dma((8,)),
            dma((10,)), dma((10,)),
            dma((10,)), dma((10,)),
            dma((7,)), dma((7,)),
        ],
        compiler_params=pltpu.CompilerParams(
            collective_id=0, has_side_effects=True, vmem_limit_bytes=48 * 1024 * 1024),
    )(*[pltpu.with_memory_space_constraint(v, pltpu.HBM) for v in (gradients, owned_rows.reshape(1, -1), master, first_moment, second_moment)])
    return pl.pallas_call(
        write,
        out_shape=(state, state, state, state, jax.ShapeDtypeStruct((ROWS, WIDTH), bf16)),
        in_specs=[vmem] * 6,
        out_specs=(hbm,) * 5,
        scratch_shapes=[dma((12,))],
        compiler_params=pltpu.CompilerParams(vmem_limit_bytes=65536),
    )(*results)


def solution(mesh):
    in_specs = (P("dp", None, None), P(), P("dp", None), P("dp", None), P("dp", None))
    out_specs = (P("dp", None), P("dp", None), P("dp", None), P("dp", None), P())
    return jax.shard_map(
        per_device, mesh=mesh, in_specs=in_specs, out_specs=out_specs, check_vma=False
    )
```
